32 devices in a mesh: owner: 4 (over x, core), rows: 8 (over z, y).
Axes of the slice: x: 2, y: 2, z: 4, core: 2. Of those that a mesh axis runs over, the one named last changes fastest.
Arguments:
- w_down: float32 [16, 6400, 4096], P('owner', None, 'rows'), may hold values from -0.109375 to 0.109375
- avg_down: bfloat16 [16, 6400, 4096], P('owner', None, 'rows'), may hold values from -0.0390625 to 0.0390625
- router_weight: float32 [4096, 16], P('rows', 'owner'), may hold values from -0.09375 to 0.09375
- router_gain: float32 [4096], P('rows'), may hold values from 0.25 to 1.75
Outputs:
- serve_down: bfloat16 [16, 6400, 4096], P('owner', 'rows')
- scale_down: float32 [16, 6400], P('owner', 'rows')
- serve_router: bfloat16 [4096, 16], replicated
The draws below stay inside these ranges and needn't reach their ends.
All inputs are finite; a program needn't handle non-finite values. Where the reference program divides by a largest or mean magnitude, that divisor is 1e-20 or more.
Results may differ from the reference program's by a relative error of at most 0.001.
Values may be sent and summed in bfloat16 or wider, within the bound.
A program may use at most 256 MiB of HBM per device.

```python
import jax
import jax.numpy as jnp

EXPERTS = 16
D_MODEL = 4096
D_EXPERT = 6400


def strengthened(values, stream_key, source, target, parts, factor):
    def block_of(position):
        return (jnp.arange(values.shape[position]) // (values.shape[position] // parts)).reshape((-1,) + (1,) * (values.ndim - 1 - position))

    one_side = jax.random.permutation(stream_key, parts)[block_of(target)]
    second = (block_of(target) + parts // 2) % parts
    return jnp.where((block_of(source) == one_side) | (block_of(source) == second), factor * values, values)


def shard_levels(rng, dims, cuts, least, high):
    loudness = 1.0
    for dim, parts in cuts:
        draws = jax.random.uniform(jax.random.fold_in(jax.random.fold_in(rng, 6), dim), (parts,), jnp.float32, least / len(cuts), high / len(cuts))
        loudness = loudness * jnp.repeat(jnp.exp(draws), dims[dim] // parts).reshape((-1,) + (1,) * (len(dims) - 1 - dim))
    return loudness


def centred(key, extent, deviation, reach, shards=(), held_as=jnp.bfloat16):
    level = shard_levels(key, extent, shards, -0.22, 0.18) if shards else 1.0
    array = jax.random.normal(key, extent, jnp.float32) * deviation * level
    return jnp.minimum(jnp.maximum(array, -reach), reach).astype(held_as)


def bell_draw_with(stream_key, dims, width, limit, shards, heavy, dtype=jnp.bfloat16):
    result = width * jax.random.normal(stream_key, dims, jnp.float32)
    if shards:
        result = result * shard_levels(stream_key, dims, shards, -0.22, 0.18)
    return jnp.clip(strengthened(result, jax.random.fold_in(stream_key, 3), *heavy), -limit, limit).astype(dtype)


def setup_inputs(seed: int = 0) -> dict:
    seeds = jax.random.split(jax.random.key(seed), 5)
    w_down = bell_draw_with(seeds[0], (EXPERTS, D_EXPERT, D_MODEL), D_EXPERT ** -0.5, 0.109375, ((0, 4), (2, 8)), (2, 1, 8, 2.0), jnp.float32)
    avg_down = centred(seeds[1], (EXPERTS, D_EXPERT, D_MODEL), (D_EXPERT * 4) ** -0.5, 0.0390625, ((0, 4), (2, 8)))
    router_weight = centred(seeds[2], (D_MODEL, EXPERTS), D_MODEL ** -0.5, 0.09375, ((0, 8), (1, 4)), jnp.float32)
    router_gain = jnp.clip(1.0 + 0.15 * jax.random.normal(seeds[3], (D_MODEL,), jnp.float32), 0.25, 1.75)
    return dict(w_down=w_down, avg_down=avg_down, router_weight=router_weight, router_gain=router_gain)


def reference(w_down, avg_down, router_weight, router_gain):
    fresh_down = w_down + avg_down.astype(jnp.float32)
    scale_down = jnp.sum(jnp.abs(fresh_down), axis=2) / D_MODEL
    serve_down = (fresh_down / jnp.expand_dims(scale_down, 2)).astype(jnp.bfloat16)
    serve_router = (router_weight * router_gain[:, None]).astype(jnp.bfloat16)
    return serve_down, scale_down, serve_router
```

```python
import functools

import jax
import jax.numpy as jnp
from jax import lax
from jax.experimental import pallas as pl
from jax.experimental.pallas import tpu as pltpu
from jax.sharding import PartitionSpec as P

LANES = 128
DEPTH = 4
VMEM_LIMIT = 38 * 1024 * 1024
MESH = pl.DeviceIdType.MESH


def pieces(low, high):
    return [(at // LANES, at, min(LANES, high - at)) for at in range(low, high, LANES)]


def kernel(n, owners, first, w_ref, a_ref, rw_ref, gain_ref, out_ref, totals, totals0, routed,
           w_buf, a_buf, staged, sums, parts, halves, sums0, parts0,
           load_sem, load0_sem, send_sem, recv_sem, sum0_send, sum0_recv,
           part_send, part_recv, half_send, half_recv, tot_send, tot_recv,
           row_send, row_recv, col_send, col_recv):
    me, mine = lax.axis_index("rows"), lax.axis_index("owner")
    experts, rows, cols = w_ref.shape
    block = rows // n
    half, quarter = n // 2, n // 4
    side, place = me // half, me % quarter
    outer = (me // quarter) % 2 == side
    inner = (me // quarter) % 2 != side
    groups = [(0, first, block)] + [(e, 0, block) for e in range(1, experts)]
    spans = [(0, 0, first)] + groups

    def peer(k):
        out, bit = 0, 1
        while bit < n:
            out = out + bit * (((me // bit) % 2 + (k // bit) % 2) % 2)
            bit *= 2
        return out

    def each_peer(fn):
        @pl.loop(1, n)
        def _(k):
            fn(peer(k))

    def each_owner(fn):
        @pl.loop(1, owners)
        def _(k):
            fn((mine + k) % owners)

    def each_outer(fn):
        @pl.loop(0, quarter)
        def _(i):
            p = side * (half + quarter) + i
            pl.when(p != me)(lambda: fn(p))

    def each_beside(fn):
        @pl.loop(1, half)
        def _(k):
            fn(peer(k))

    barrier = pltpu.get_barrier_semaphore()
    each_peer(lambda p: pl.semaphore_signal(barrier, inc=1, device_id={"rows": p}, device_id_type=MESH))
    each_owner(lambda q: pl.semaphore_signal(barrier, inc=1, device_id={"owner": q}, device_id_type=MESH))

    def rows_of(p, low, count):
        return pl.ds(pl.multiple_of(p * block + low, 16), count)

    def first_loads(k):
        span = rows_of(peer(k), 0, first)
        to = pl.ds(pl.multiple_of((k % 2) * first, LANES), first)
        return (pltpu.make_async_copy(w_ref.at[0, span], w_buf.at[k // 2, to], load0_sem.at[0, k]),
                pltpu.make_async_copy(a_ref.at[0, span], a_buf.at[k // 2, to], load0_sem.at[1, k]))

    def loads(e, low, high, step):
        slot, span, to = step % DEPTH, rows_of(peer(order(step)), low, high - low), pl.ds(0, high - low)
        return (pltpu.make_async_copy(w_ref.at[e, span], w_buf.at[slot, to], load_sem.at[0, slot]),
                pltpu.make_async_copy(a_ref.at[e, span], a_buf.at[slot, to], load_sem.at[1, slot]))

    def order(step):
        return (step + half) % n

    def prime(group):
        for step in range(min(DEPTH - 1, n)):
            for copy in loads(*group, step):
                copy.start()

    def stream(group, body):
        @pl.loop(0, n)
        def _(step):
            for copy in loads(*group, step):
                copy.wait()

            @pl.when(step + (DEPTH - 1) < n)
            def _():
                for copy in loads(*group, step + (DEPTH - 1)):
                    copy.start()

            body(order(step), step)

    def fresh(slot, span, c):
        return w_buf[slot, span, c:c + LANES] + a_buf[slot, span, c:c + LANES].astype(jnp.float32)

    def row_sums(slot, span):
        acc = None
        for c in range(0, cols, LANES):
            f = jnp.abs(fresh(slot, span, c))
            acc = f if acc is None else acc + f
        return jnp.sum(acc.T, axis=0, keepdims=True)

    def narrow(e, low, high, k, slot, start, total):
        p = peer(k)

        def write(put):
            for j, at, size in pieces(low, high):
                factor = jnp.broadcast_to(1.0 / total(p, j), (LANES, LANES)).T[:size]
                span = pl.ds(pl.multiple_of(start + (at - low), LANES), size)
                for c in range(0, cols, LANES):
                    put(at, size, c, (fresh(slot, span, c) * factor).astype(jnp.bfloat16))

        def keep(at, size, c, value):
            out_ref[e, at:at + size, pl.ds(pl.multiple_of(me * cols + c, LANES), LANES)] = value

        def stage(at, size, c, value):
            staged[e, rows_of(p, at, size), c:c + LANES] = value

        pl.when(k == 0)(lambda: write(keep))
        pl.when(k != 0)(lambda: write(stage))

    def block_copy(part, p, source):
        e, low, high = spans[part]
        return pltpu.make_async_remote_copy(
            src_ref=staged.at[e, rows_of(p, low, high - low)],
            dst_ref=out_ref.at[e, pl.ds(low, high - low), pl.ds(pl.multiple_of(source * cols, LANES), cols)],
            send_sem=send_sem.at[part, p], recv_sem=recv_sem.at[part, source],
            device_id={"rows": p}, device_id_type=MESH)

    def first_copy(p, source):
        return pltpu.make_async_remote_copy(
            src_ref=sums0, dst_ref=parts0.at[source],
            send_sem=sum0_send.at[p], recv_sem=sum0_recv.at[source],
            device_id={"rows": p}, device_id_type=MESH)

    def part_copy(g, p, source):
        e = groups[g][0]
        return pltpu.make_async_remote_copy(
            src_ref=sums.at[:, p % quarter, e], dst_ref=parts.at[source % half, :, e],
            send_sem=part_send.at[g, p % quarter], recv_sem=part_recv.at[g, source % half],
            device_id={"rows": p}, device_id_type=MESH)

    def half_copy(g):
        e = groups[g][0]
        return pltpu.make_async_remote_copy(
            src_ref=halves.at[0, :, e], dst_ref=halves.at[1, :, e],
            send_sem=half_send.at[g], recv_sem=half_recv.at[g],
            device_id={"rows": peer(half + quarter)}, device_id_type=MESH)

    def total_copy(g, p, source):
        e, at = groups[g][0], source % quarter
        return pltpu.make_async_remote_copy(
            src_ref=totals.at[:, at, e], dst_ref=totals.at[:, at, e],
            send_sem=tot_send.at[g, p % half], recv_sem=tot_recv.at[g, at],
            device_id={"rows": p}, device_id_type=MESH)

    def send_sums(g):
        each_outer(lambda p: part_copy(g, p, me).start())

    def cross_sums(g):
        @pl.when(outer)
        def _():
            e = groups[g][0]
            parts[me % half, :, e] = sums[:, place, e]
            each_beside(lambda p: part_copy(g, p, p).wait_recv())
            total = parts[0, :, e]
            for r in range(1, half):
                total = total + parts[r, :, e]
            halves[0, :, e] = total
            half_copy(g).start()

    def send_totals(g):
        @pl.when(outer)
        def _():
            e = groups[g][0]
            half_copy(g).wait_recv()
            totals[:, place, e] = (halves[0, :, e] + halves[1, :, e]) / (cols * n)
            each_beside(lambda p: total_copy(g, p, me).start())

    def take_totals(g):
        each_outer(lambda p: total_copy(g, p, p).wait_recv())

    def row_copy(p, source):
        return pltpu.make_async_remote_copy(
            src_ref=routed.at[mine, source], dst_ref=routed.at[mine, source],
            send_sem=row_send.at[p], recv_sem=row_recv.at[source],
            device_id={"rows": p}, device_id_type=MESH)

    def col_copy(q, source):
        return pltpu.make_async_remote_copy(
            src_ref=routed.at[source], dst_ref=routed.at[source],
            send_sem=col_send.at[q], recv_sem=col_recv.at[source],
            device_id={"owner": q}, device_id_type=MESH)

    def send_crossing(part, k):
        @pl.when(inner & (k >= half))
        def _():
            block_copy(part, peer(k), me).start()

    @pl.loop(0, n)
    def _(k):
        for copy in first_loads(k):
            copy.start()

    sums[...] = jnp.zeros_like(sums)
    routed[mine, me] = (rw_ref[...] * gain_ref[...]).astype(jnp.bfloat16)

    @pl.loop(0, n)
    def _(k):
        for copy in first_loads(k):
            copy.wait()
        for j, at, size in pieces(0, first):
            span = pl.ds(pl.multiple_of((k % 2) * first + at, LANES), size)
            sums0[j, pl.ds(peer(k), 1), :] = row_sums(k // 2, span)

    pl.semaphore_wait(barrier, n - 1 + owners - 1)
    each_peer(lambda p: first_copy(p, me).start())
    parts0[me] = sums0[...]
    each_peer(lambda p: row_copy(p, me).start())
    each_peer(lambda p: first_copy(p, p).wait_recv())
    total = parts0[0]
    for r in range(1, n):
        total = total + parts0[r]
    totals0[...] = total / (cols * n)

    @pl.loop(0, n)
    def _(step):
        k = order(step)
        narrow(0, 0, first, k, k // 2, (k % 2) * first, lambda p, j: totals0[j, pl.ds(p, 1), :])
        send_crossing(0, k)

    def add_up(g, behind):
        e, low, high = groups[g]

        def body(k, step):
            p = peer(k)
            for j, at, size in pieces(low, high):
                sums[p // quarter, p % quarter, e, j:j + 1, 0:size] = row_sums(step % DEPTH, pl.ds(at - low, size))
            if behind is not None:
                pl.when(step == n // 2 - 1)(lambda: cross_sums(behind))
                pl.when(step == n - 1)(lambda: send_totals(behind))

        stream(groups[g], body)

    def narrow_all(g):
        e, low, high = groups[g]

        def body(k, step):
            narrow(e, low, high, k, step % DEPTH, 0,
                   lambda p, j: totals[p // quarter, p % quarter, e, j:j + 1, :])
            send_crossing(g + 1, k)

        stream(groups[g], body)

    prime(groups[0])
    add_up(0, None)
    for g in range(experts):
        send_sums(g)
        if g + 1 < experts:
            prime(groups[g + 1])
            add_up(g + 1, g)
        else:
            cross_sums(g)
            send_totals(g)
        prime(groups[g])
        take_totals(g)
        narrow_all(g)

    for part in range(experts + 1):
        each_beside(lambda p, part=part: block_copy(part, p, me).start())

    each_peer(lambda p: row_copy(p, p).wait_recv())
    each_owner(lambda q: col_copy(q, mine).start())

    @pl.when(outer)
    def _():
        for part in range(experts + 1):
            @pl.loop(half, n)
            def _(k, part=part):
                block_copy(part, peer(k), me).start()

    each_owner(lambda q: col_copy(q, q).wait_recv())
    each_owner(lambda q: col_copy(q, mine).wait_send())
    each_peer(lambda p: row_copy(p, me).wait_send())
    each_peer(lambda p: first_copy(p, me).wait_send())
    for g in range(experts):
        each_outer(lambda p, g=g: part_copy(g, p, me).wait_send())

        @pl.when(outer)
        def _(g=g):
            half_copy(g).wait_send()
            each_beside(lambda p: total_copy(g, p, me).wait_send())
    for part in range(experts + 1):
        each_peer(lambda p, part=part: block_copy(part, p, me).wait_send())
        each_peer(lambda p, part=part: block_copy(part, p, p).wait_recv())


def finish(first, held, totals, totals0, routed, out_ref, scale_ref, router_ref, scale, wide, router, out_sem, sem):
    me = lax.axis_index("rows")
    experts, block, _ = held.shape
    owners, n, few, cols = routed.shape
    quarter = totals.shape[1]
    outs = [pltpu.make_async_copy(held.at[e], out_ref.at[e], out_sem.at[e]) for e in range(experts)]
    for copy in outs:
        copy.start()
    for e in range(experts):
        for j, at, size in pieces(0, block):
            if e == 0 and at < first:
                row = totals0[j, pl.ds(me, 1), :]
            else:
                row = totals[me // quarter, me % quarter, e, j:j + 1, 0:size]
            scale[e:e + 1, at:at + size] = row
    for q in range(owners):
        for r in range(n):
            wide[q * few:(q + 1) * few, r * cols:(r + 1) * cols] = routed[q, r].astype(jnp.float32)
    router[...] = wide[...].astype(jnp.bfloat16)
    small = [pltpu.make_async_copy(scale, scale_ref, sem.at[0]), pltpu.make_async_copy(router, router_ref, sem.at[1])]
    for copy in small:
        copy.start()
    for copy in small + outs:
        copy.wait()


def with_kernel(n, owners, w_down, avg_down, router_weight, router_gain):
    experts, rows, cols = w_down.shape
    few = router_weight.shape[1]
    block = rows // n
    half, quarter = n // 2, n // 4
    piece = -(-block // LANES)
    first = LANES * min(2, (block - 1) // LANES)
    dma = pltpu.SemaphoreType.DMA
    anywhere, vmem = pl.BlockSpec(memory_space=pl.ANY), pl.BlockSpec(memory_space=pltpu.VMEM)
    sums = pltpu.VMEM((4, quarter, experts, piece, LANES), jnp.float32)
    sums0 = pltpu.VMEM((first // LANES, n, LANES), jnp.float32)
    held = pl.pallas_call(
        functools.partial(kernel, n, owners, first),
        out_shape=(
            pltpu.VMEM((experts, block, cols * n), jnp.bfloat16),
            sums,
            sums0,
            pltpu.VMEM((owners, n, few, cols), jnp.bfloat16),
        ),
        in_specs=[anywhere] * 2 + [vmem] * 2,
        out_specs=(vmem,) * 4,
        scratch_shapes=[
            pltpu.VMEM((DEPTH, block, cols), jnp.float32),
            pltpu.VMEM((DEPTH, block, cols), jnp.bfloat16),
            pltpu.VMEM((experts, rows, cols), jnp.bfloat16),
            sums,
            pltpu.VMEM((half, 4, experts, piece, LANES), jnp.float32),
            pltpu.VMEM((2, 4, experts, piece, LANES), jnp.float32),
            sums0,
            pltpu.VMEM((n, first // LANES, n, LANES), jnp.float32),
            dma((2, DEPTH)), dma((2, n)),
            dma((experts + 1, n)), dma((experts + 1, n)),
            dma((n,)), dma((n,)),
            dma((experts, quarter)), dma((experts, half)), dma((experts,)), dma((experts,)),
            dma((experts, half)), dma((experts, quarter)),
            dma((n,)), dma((n,)), dma((owners,)), dma((owners,)),
        ],
        compiler_params=pltpu.CompilerParams(
            collective_id=0, has_side_effects=True, vmem_limit_bytes=VMEM_LIMIT
        ),
        name="serve",
    )(w_down, avg_down, router_weight.T, router_gain[None, :])
    out, scales, router = pl.pallas_call(
        functools.partial(finish, first),
        out_shape=(
            jax.ShapeDtypeStruct((experts, block, cols * n), jnp.bfloat16),
            jax.ShapeDtypeStruct((experts, block), jnp.float32),
            jax.ShapeDtypeStruct((owners * few, cols * n), jnp.bfloat16),
        ),
        in_specs=[vmem] * 4,
        out_specs=(anywhere,) * 3,
        scratch_shapes=[
            pltpu.VMEM((experts, block), jnp.float32),
            pltpu.VMEM((owners * few, cols * n), jnp.float32),
            pltpu.VMEM((owners * few, cols * n), jnp.bfloat16),
            dma((experts,)), dma((2,)),
        ],
        compiler_params=pltpu.CompilerParams(vmem_limit_bytes=4 * 1024 * 1024),
        name="finish",
    )(*held)
    return out, scales, router.T


def with_collectives(n, owners, w_down, avg_down, router_weight, router_gain):
    fresh = w_down + avg_down.astype(jnp.float32)
    scales = lax.psum(jnp.sum(jnp.abs(fresh), axis=2), "rows") / (w_down.shape[2] * n)
    narrow = (fresh / jnp.expand_dims(scales, 2)).astype(jnp.bfloat16)
    out = lax.all_to_all(narrow, "rows", split_axis=1, concat_axis=2, tiled=True)
    scales = lax.dynamic_slice_in_dim(scales, lax.axis_index("rows") * out.shape[1], out.shape[1], axis=1)
    part = (router_weight * router_gain[:, None]).astype(jnp.bfloat16)
    router = lax.all_gather(lax.all_gather(part, "rows", axis=0, tiled=True), "owner", axis=1, tiled=True)
    return out, scales, router


def solution(mesh):
    n, owners = mesh.shape["rows"], mesh.shape["owner"]

    def per_device(w_down, avg_down, router_weight, router_gain):
        experts, rows, cols = w_down.shape
        fits = n >= 4 and (n & (n - 1)) == 0 and rows // n > LANES and rows % LANES == 0 and rows % (16 * n) == 0 and cols % LANES == 0
        path = with_kernel if fits else with_collectives
        return path(n, owners, w_down, avg_down, router_weight, router_gain)

    return jax.shard_map(
        per_device,
        mesh=mesh,
        in_specs=(
            P("owner", None, "rows"),
            P("owner", None, "rows"),
            P("rows", "owner"),
            P("rows"),
        ),
        out_specs=(P("owner", "rows", None), P("owner", "rows"), P()),
        check_vma=False,
    )
```

```python
import functools

import jax
import jax.numpy as jnp
from jax import lax
from jax.experimental import pallas as pl
from jax.experimental.pallas import tpu as pltpu
from jax.sharding import PartitionSpec as P

LANES = 128
DEPTH = 4
VMEM_LIMIT = 38 * 1024 * 1024
MESH = pl.DeviceIdType.MESH


def pieces(low, high):
    return [(at // LANES, at, min(LANES, high - at)) for at in range(low, high, LANES)]


def kernel(n, owners, first, w_ref, a_ref, rw_ref, gain_ref, out_ref, totals, totals0, routed,
           w_buf, a_buf, staged, sums, parts, halves, sums0, parts0,
           load_sem, load0_sem, send_sem, recv_sem, sum0_send, sum0_recv,
           part_send, part_recv, half_send, half_recv, tot_send, tot_recv,
           row_send, row_recv, col_send, col_recv):
    me, mine = lax.axis_index("rows"), lax.axis_index("owner")
    experts, rows, cols = w_ref.shape
    block = rows // n
    half, quarter = n // 2, n // 4
    side, place = me // half, me % quarter
    outer = (me // quarter) % 2 == side
    inner = (me // quarter) % 2 != side
    turn = (mine % 2) * quarter
    groups = [(0, first, block)] + [(e, 0, block) for e in range(1, experts)]
    spans = [(0, 0, first)] + groups

    def peer(k):
        out, bit = 0, 1
        while bit < n:
            out = out + bit * (((me // bit) % 2 + (k // bit) % 2) % 2)
            bit *= 2
        return out

    def each_peer(fn):
        @pl.loop(1, n)
        def _(k):
            fn(peer(k))

    def each_owner(fn):
        @pl.loop(1, owners)
        def _(k):
            fn((mine + k) % owners)

    def each_outer(fn):
        @pl.loop(0, quarter)
        def _(i):
            p = side * (half + quarter) + i
            pl.when(p != me)(lambda: fn(p))

    def each_beside(fn):
        @pl.loop(1, half)
        def _(k):
            fn(peer(k))

    barrier = pltpu.get_barrier_semaphore()
    each_peer(lambda p: pl.semaphore_signal(barrier, inc=1, device_id={"rows": p}, device_id_type=MESH))
    each_owner(lambda q: pl.semaphore_signal(barrier, inc=1, device_id={"owner": q}, device_id_type=MESH))

    def rows_of(p, low, count):
        return pl.ds(pl.multiple_of(p * block + low, 16), count)

    def first_loads(k):
        span = rows_of(peer(k), 0, first)
        to = pl.ds(pl.multiple_of((k % 2) * first, LANES), first)
        return (pltpu.make_async_copy(w_ref.at[0, span], w_buf.at[k // 2, to], load0_sem.at[0, k]),
                pltpu.make_async_copy(a_ref.at[0, span], a_buf.at[k // 2, to], load0_sem.at[1, k]))

    def loads(e, low, high, step):
        slot, span, to = step % DEPTH, rows_of(peer(order(step)), low, high - low), pl.ds(0, high - low)
        return (pltpu.make_async_copy(w_ref.at[e, span], w_buf.at[slot, to], load_sem.at[0, slot]),
                pltpu.make_async_copy(a_ref.at[e, span], a_buf.at[slot, to], load_sem.at[1, slot]))

    def order(step):
        return jnp.where(step < half, half + (step + turn) % half, step - half)

    def prime(group):
        for step in range(min(DEPTH - 1, n)):
            for copy in loads(*group, step):
                copy.start()

    def stream(group, body):
        @pl.loop(0, n)
        def _(step):
            for copy in loads(*group, step):
                copy.wait()

            @pl.when(step + (DEPTH - 1) < n)
            def _():
                for copy in loads(*group, step + (DEPTH - 1)):
                    copy.start()

            body(order(step), step)

    def fresh(slot, span, c):
        return w_buf[slot, span, c:c + LANES] + a_buf[slot, span, c:c + LANES].astype(jnp.float32)

    def row_sums(slot, span):
        acc = None
        for c in range(0, cols, LANES):
            f = jnp.abs(fresh(slot, span, c))
            acc = f if acc is None else acc + f
        return jnp.sum(acc.T, axis=0, keepdims=True)

    def narrow(e, low, high, k, slot, start, total):
        p = peer(k)

        def write(put):
            for j, at, size in pieces(low, high):
                factor = jnp.broadcast_to(1.0 / total(p, j), (LANES, LANES)).T[:size]
                span = pl.ds(pl.multiple_of(start + (at - low), LANES), size)
                for c in range(0, cols, LANES):
                    put(at, size, c, (fresh(slot, span, c) * factor).astype(jnp.bfloat16))

        def keep(at, size, c, value):
            out_ref[e, at:at + size, pl.ds(pl.multiple_of(me * cols + c, LANES), LANES)] = value

        def stage(at, size, c, value):
            staged[e, rows_of(p, at, size), c:c + LANES] = value

        pl.when(k == 0)(lambda: write(keep))
        pl.when(k != 0)(lambda: write(stage))

    def block_copy(part, p, source):
        e, low, high = spans[part]
        return pltpu.make_async_remote_copy(
            src_ref=staged.at[e, rows_of(p, low, high - low)],
            dst_ref=out_ref.at[e, pl.ds(low, high - low), pl.ds(pl.multiple_of(source * cols, LANES), cols)],
            send_sem=send_sem.at[part, p], recv_sem=recv_sem.at[part, source],
            device_id={"rows": p}, device_id_type=MESH)

    def first_copy(p, source):
        return pltpu.make_async_remote_copy(
            src_ref=sums0, dst_ref=parts0.at[source],
            send_sem=sum0_send.at[p], recv_sem=sum0_recv.at[source],
            device_id={"rows": p}, device_id_type=MESH)

    def part_copy(g, p, source):
        e = groups[g][0]
        return pltpu.make_async_remote_copy(
            src_ref=sums.at[:, p % quarter, e], dst_ref=parts.at[source % half, :, e],
            send_sem=part_send.at[g, p % quarter], recv_sem=part_recv.at[g, source % half],
            device_id={"rows": p}, device_id_type=MESH)

    def half_copy(g):
        e = groups[g][0]
        return pltpu.make_async_remote_copy(
            src_ref=halves.at[0, :, e], dst_ref=halves.at[1, :, e],
            send_sem=half_send.at[g], recv_sem=half_recv.at[g],
            device_id={"rows": peer(half + quarter)}, device_id_type=MESH)

    def total_copy(g, p, source):
        e, at = groups[g][0], source % quarter
        return pltpu.make_async_remote_copy(
            src_ref=totals.at[:, at, e], dst_ref=totals.at[:, at, e],
            send_sem=tot_send.at[g, p % half], recv_sem=tot_recv.at[g, at],
            device_id={"rows": p}, device_id_type=MESH)

    def send_sums(g):
        each_outer(lambda p: part_copy(g, p, me).start())

    def cross_sums(g):
        @pl.when(outer)
        def _():
            e = groups[g][0]
            parts[me % half, :, e] = sums[:, place, e]
            each_beside(lambda p: part_copy(g, p, p).wait_recv())
            total = parts[0, :, e]
            for r in range(1, half):
                total = total + parts[r, :, e]
            halves[0, :, e] = total
            half_copy(g).start()

    def send_totals(g):
        @pl.when(outer)
        def _():
            e = groups[g][0]
            half_copy(g).wait_recv()
            totals[:, place, e] = (halves[0, :, e] + halves[1, :, e]) / (cols * n)
            each_beside(lambda p: total_copy(g, p, me).start())

    def take_totals(g):
        each_outer(lambda p: total_copy(g, p, p).wait_recv())

    def row_copy(p, source):
        return pltpu.make_async_remote_copy(
            src_ref=routed.at[mine, source], dst_ref=routed.at[mine, source],
            send_sem=row_send.at[p], recv_sem=row_recv.at[source],
            device_id={"rows": p}, device_id_type=MESH)

    def col_copy(q, source):
        return pltpu.make_async_remote_copy(
            src_ref=routed.at[source], dst_ref=routed.at[source],
            send_sem=col_send.at[q], recv_sem=col_recv.at[source],
            device_id={"owner": q}, device_id_type=MESH)

    def send_crossing(part, k):
        @pl.when(inner & (k >= half) & ((k - half) // quarter == mine % 2 if part else True))
        def _():
            block_copy(part, peer(k), me).start()

    def send_late(parts, low, high):
        for part in parts:
            @pl.loop(low, high)
            def _(k, part=part):
                block_copy(part, peer(k), me).start()

    @pl.loop(0, n)
    def _(k):
        for copy in first_loads(k):
            copy.start()

    sums[...] = jnp.zeros_like(sums)
    routed[mine, me] = (rw_ref[...] * gain_ref[...]).astype(jnp.bfloat16)

    @pl.loop(0, n)
    def _(k):
        for copy in first_loads(k):
            copy.wait()
        for j, at, size in pieces(0, first):
            span = pl.ds(pl.multiple_of((k % 2) * first + at, LANES), size)
            sums0[j, pl.ds(peer(k), 1), :] = row_sums(k // 2, span)

    pl.semaphore_wait(barrier, n - 1 + owners - 1)
    each_peer(lambda p: first_copy(p, me).start())
    parts0[me] = sums0[...]
    each_peer(lambda p: row_copy(p, me).start())
    each_peer(lambda p: first_copy(p, p).wait_recv())
    total = parts0[0]
    for r in range(1, n):
        total = total + parts0[r]
    totals0[...] = total / (cols * n)

    @pl.loop(0, n)
    def _(step):
        k = order(step)
        narrow(0, 0, first, k, k // 2, (k % 2) * first, lambda p, j: totals0[j, pl.ds(p, 1), :])
        send_crossing(0, k)

    def add_up(g, behind):
        e, low, high = groups[g]

        def body(k, step):
            p = peer(k)
            for j, at, size in pieces(low, high):
                sums[p // quarter, p % quarter, e, j:j + 1, 0:size] = row_sums(step % DEPTH, pl.ds(at - low, size))
            if behind is not None:
                pl.when(step == n // 2 - 1)(lambda: cross_sums(behind))
                pl.when(step == n - 1)(lambda: send_totals(behind))

        stream(groups[g], body)

    def narrow_all(g):
        e, low, high = groups[g]

        def body(k, step):
            narrow(e, low, high, k, step % DEPTH, 0,
                   lambda p, j: totals[p // quarter, p % quarter, e, j:j + 1, :])
            send_crossing(g + 1, k)

        stream(groups[g], body)

    prime(groups[0])
    add_up(0, None)
    for g in range(experts):
        send_sums(g)
        if g + 1 < experts:
            prime(groups[g + 1])
            add_up(g + 1, g)
        else:
            cross_sums(g)
            send_totals(g)
        prime(groups[g])
        take_totals(g)
        narrow_all(g)

    @pl.when(inner)
    def _():
        send_late(range(1, experts + 1), half + quarter - turn, n - turn)

    send_late(range(experts + 1), 1, half)

    each_peer(lambda p: row_copy(p, p).wait_recv())
    each_owner(lambda q: col_copy(q, mine).start())

    @pl.when(outer)
    def _():
        send_late(range(experts + 1), half + turn, half + quarter + turn)
        send_late(range(experts + 1), half + quarter - turn, n - turn)

    each_owner(lambda q: col_copy(q, q).wait_recv())
    each_owner(lambda q: col_copy(q, mine).wait_send())
    each_peer(lambda p: row_copy(p, me).wait_send())
    each_peer(lambda p: first_copy(p, me).wait_send())
    for g in range(experts):
        each_outer(lambda p, g=g: part_copy(g, p, me).wait_send())

        @pl.when(outer)
        def _(g=g):
            half_copy(g).wait_send()
            each_beside(lambda p: total_copy(g, p, me).wait_send())
    for part in range(experts + 1):
        each_peer(lambda p, part=part: block_copy(part, p, me).wait_send())
        each_peer(lambda p, part=part: block_copy(part, p, p).wait_recv())


def finish(first, held, totals, totals0, routed, out_ref, scale_ref, router_ref, scale, wide, router, out_sem, sem):
    me = lax.axis_index("rows")
    experts, block, _ = held.shape
    owners, n, few, cols = routed.shape
    quarter = totals.shape[1]
    outs = [pltpu.make_async_copy(held.at[e], out_ref.at[e], out_sem.at[e]) for e in range(experts)]
    for copy in outs:
        copy.start()
    for e in range(experts):
        for j, at, size in pieces(0, block):
            if e == 0 and at < first:
                row = totals0[j, pl.ds(me, 1), :]
            else:
                row = totals[me // quarter, me % quarter, e, j:j + 1, 0:size]
            scale[e:e + 1, at:at + size] = row
    for q in range(owners):
        for r in range(n):
            wide[q * few:(q + 1) * few, r * cols:(r + 1) * cols] = routed[q, r].astype(jnp.float32)
    router[...] = wide[...].astype(jnp.bfloat16)
    small = [pltpu.make_async_copy(scale, scale_ref, sem.at[0]), pltpu.make_async_copy(router, router_ref, sem.at[1])]
    for copy in small:
        copy.start()
    for copy in small + outs:
        copy.wait()


def with_kernel(n, owners, w_down, avg_down, router_weight, router_gain):
    experts, rows, cols = w_down.shape
    few = router_weight.shape[1]
    block = rows // n
    half, quarter = n // 2, n // 4
    piece = -(-block // LANES)
    first = LANES * min(2, (block - 1) // LANES)
    dma = pltpu.SemaphoreType.DMA
    anywhere, vmem = pl.BlockSpec(memory_space=pl.ANY), pl.BlockSpec(memory_space=pltpu.VMEM)
    sums = pltpu.VMEM((4, quarter, experts, piece, LANES), jnp.float32)
    sums0 = pltpu.VMEM((first // LANES, n, LANES), jnp.float32)
    held = pl.pallas_call(
        functools.partial(kernel, n, owners, first),
        out_shape=(
            pltpu.VMEM((experts, block, cols * n), jnp.bfloat16),
            sums,
            sums0,
            pltpu.VMEM((owners, n, few, cols), jnp.bfloat16),
        ),
        in_specs=[anywhere] * 2 + [vmem] * 2,
        out_specs=(vmem,) * 4,
        scratch_shapes=[
            pltpu.VMEM((DEPTH, block, cols), jnp.float32),
            pltpu.VMEM((DEPTH, block, cols), jnp.bfloat16),
            pltpu.VMEM((experts, rows, cols), jnp.bfloat16),
            sums,
            pltpu.VMEM((half, 4, experts, piece, LANES), jnp.float32),
            pltpu.VMEM((2, 4, experts, piece, LANES), jnp.float32),
            sums0,
            pltpu.VMEM((n, first // LANES, n, LANES), jnp.float32),
            dma((2, DEPTH)), dma((2, n)),
            dma((experts + 1, n)), dma((experts + 1, n)),
            dma((n,)), dma((n,)),
            dma((experts, quarter)), dma((experts, half)), dma((experts,)), dma((experts,)),
            dma((experts, half)), dma((experts, quarter)),
            dma((n,)), dma((n,)), dma((owners,)), dma((owners,)),
        ],
        compiler_params=pltpu.CompilerParams(
            collective_id=0, has_side_effects=True, vmem_limit_bytes=VMEM_LIMIT
        ),
        name="serve",
    )(w_down, avg_down, router_weight.T, router_gain[None, :])
    out, scales, router = pl.pallas_call(
        functools.partial(finish, first),
        out_shape=(
            jax.ShapeDtypeStruct((experts, block, cols * n), jnp.bfloat16),
            jax.ShapeDtypeStruct((experts, block), jnp.float32),
            jax.ShapeDtypeStruct((owners * few, cols * n), jnp.bfloat16),
        ),
        in_specs=[vmem] * 4,
        out_specs=(anywhere,) * 3,
        scratch_shapes=[
            pltpu.VMEM((experts, block), jnp.float32),
            pltpu.VMEM((owners * few, cols * n), jnp.float32),
            pltpu.VMEM((owners * few, cols * n), jnp.bfloat16),
            dma((experts,)), dma((2,)),
        ],
        compiler_params=pltpu.CompilerParams(vmem_limit_bytes=4 * 1024 * 1024),
        name="finish",
    )(*held)
    return out, scales, router.T


def with_collectives(n, owners, w_down, avg_down, router_weight, router_gain):
    fresh = w_down + avg_down.astype(jnp.float32)
    scales = lax.psum(jnp.sum(jnp.abs(fresh), axis=2), "rows") / (w_down.shape[2] * n)
    narrow = (fresh / jnp.expand_dims(scales, 2)).astype(jnp.bfloat16)
    out = lax.all_to_all(narrow, "rows", split_axis=1, concat_axis=2, tiled=True)
    scales = lax.dynamic_slice_in_dim(scales, lax.axis_index("rows") * out.shape[1], out.shape[1], axis=1)
    part = (router_weight * router_gain[:, None]).astype(jnp.bfloat16)
    router = lax.all_gather(lax.all_gather(part, "rows", axis=0, tiled=True), "owner", axis=1, tiled=True)
    return out, scales, router


def solution(mesh):
    n, owners = mesh.shape["rows"], mesh.shape["owner"]

    def per_device(w_down, avg_down, router_weight, router_gain):
        experts, rows, cols = w_down.shape
        fits = n >= 4 and (n & (n - 1)) == 0 and rows // n > LANES and rows % LANES == 0 and rows % (16 * n) == 0 and cols % LANES == 0
        path = with_kernel if fits else with_collectives
        return path(n, owners, w_down, avg_down, router_weight, router_gain)

    return jax.shard_map(
        per_device,
        mesh=mesh,
        in_specs=(
            P("owner", None, "rows"),
            P("owner", None, "rows"),
            P("rows", "owner"),
            P("rows"),
        ),
        out_specs=(P("owner", "rows", None), P("owner", "rows"), P()),
        check_vma=False,
    )
```

```python
import functools

import jax
import jax.numpy as jnp
from jax import lax
from jax.experimental import pallas as pl
from jax.experimental.pallas import tpu as pltpu
from jax.sharding import PartitionSpec as P

LANES = 128
DEPTH = 4
VMEM_LIMIT = 36 * 1024 * 1024
MESH = pl.DeviceIdType.MESH


def pieces(low, high):
    return [(at // LANES, at, min(LANES, high - at)) for at in range(low, high, LANES)]


def flipped(n, me, k):
    out, bit = 0, 1
    while bit < n:
        out = out + bit * (((me // bit) % 2 + (k // bit) % 2) % 2)
        bit *= 2
    return out


def kernel(n, owners, first, cuts, w_ref, a_ref, rw_ref, gain_ref, out_ref, totals, totals0, routed, kept,
           w_buf, a_buf, staged, sums, parts, halves, sums0, parts0,
           load_sem, load0_sem, send_sem, recv_sem, sum0_send, sum0_recv,
           part_send, part_recv, half_send, half_recv, tot_send, tot_recv,
           row_send, row_recv, col_send, col_recv, turn_sem):
    me, mine = lax.axis_index("rows"), lax.axis_index("owner")
    experts, rows, cols = w_ref.shape
    block = rows // n
    half, quarter = n // 2, n // 4
    side, place = me // half, me % quarter
    outer = (me // quarter) % 2 == side
    inner = (me // quarter) % 2 != side
    turn = (mine % 2) * quarter
    groups = [(0, first, block)] + [(e, 0, block) for e in range(1, experts)]
    e = experts - 1
    last = experts + 3
    spans = [(0, 0, first)] + groups[:-1] + [(e, low, high) for low, high in zip((groups[-1][1],) + cuts, cuts + (block,))]
    parts_of = lambda g: range(experts, last + 1) if g == experts - 1 else [g + 1]

    def peer(k):
        return flipped(n, me, k)

    def each_peer(fn):
        @pl.loop(1, n)
        def _(k):
            fn(peer(k))

    def each_owner(fn):
        @pl.loop(1, owners)
        def _(k):
            fn((mine + k) % owners)

    def each_outer(fn):
        @pl.loop(0, quarter)
        def _(i):
            p = side * (half + quarter) + i
            pl.when(p != me)(lambda: fn(p))

    def each_beside(fn):
        @pl.loop(1, half)
        def _(k):
            fn(peer(k))

    barrier = pltpu.get_barrier_semaphore()
    each_peer(lambda p: pl.semaphore_signal(barrier, inc=1, device_id={"rows": p}, device_id_type=MESH))
    each_owner(lambda q: pl.semaphore_signal(barrier, inc=1, device_id={"owner": q}, device_id_type=MESH))

    def rows_of(p, low, count):
        return pl.ds(pl.multiple_of(p * block + low, 16), count)

    def first_loads(k):
        span = rows_of(peer(k), 0, first)
        to = pl.ds(pl.multiple_of((k % 2) * first, LANES), first)
        return (pltpu.make_async_copy(w_ref.at[0, span], w_buf.at[k // 2, to], load0_sem.at[0, k]),
                pltpu.make_async_copy(a_ref.at[0, span], a_buf.at[k // 2, to], load0_sem.at[1, k]))

    def loads(e, low, high, step):
        slot, span, to = step % DEPTH, rows_of(peer(order(step)), low, high - low), pl.ds(0, high - low)
        return (pltpu.make_async_copy(w_ref.at[e, span], w_buf.at[slot, to], load_sem.at[0, slot]),
                pltpu.make_async_copy(a_ref.at[e, span], a_buf.at[slot, to], load_sem.at[1, slot]))

    def order(step):
        return jnp.where(step < half, half + (step + turn) % half, step - half)

    def prime(group):
        for step in range(min(DEPTH - 1, n)):
            for copy in loads(*group, step):
                copy.start()

    def stream(group, body):
        @pl.loop(0, n)
        def _(step):
            for copy in loads(*group, step):
                copy.wait()

            @pl.when(step + (DEPTH - 1) < n)
            def _():
                for copy in loads(*group, step + (DEPTH - 1)):
                    copy.start()

            body(order(step), step)

    def fresh(slot, span, c):
        return w_buf[slot, span, c:c + LANES] + a_buf[slot, span, c:c + LANES].astype(jnp.float32)

    def row_sums(slot, span):
        acc = None
        for c in range(0, cols, LANES):
            f = jnp.abs(fresh(slot, span, c))
            acc = f if acc is None else acc + f
        return jnp.sum(acc.T, axis=0, keepdims=True)

    def narrow(e, low, high, k, slot, start, total):
        p = peer(k)

        def write(put):
            for j, at, size in pieces(low, high):
                factor = jnp.broadcast_to(1.0 / total(p, j), (LANES, LANES)).T[:size]
                span = pl.ds(pl.multiple_of(start + (at - low), LANES), size)
                for c in range(0, cols, LANES):
                    put(at, size, c, (fresh(slot, span, c) * factor).astype(jnp.bfloat16))

        def keep(at, size, c, value):
            out_ref[e, at:at + size, pl.ds(pl.multiple_of(me * cols + c, LANES), LANES)] = value

        def stage(at, size, c, value):
            staged[e, rows_of(p, at, size), c:c + LANES] = value

        pl.when(k == 0)(lambda: write(keep))
        pl.when(k != 0)(lambda: write(stage))

    def block_copy(part, p, source):
        e, low, high = spans[part]
        return pltpu.make_async_remote_copy(
            src_ref=staged.at[e, rows_of(p, low, high - low)],
            dst_ref=out_ref.at[e, pl.ds(low, high - low), pl.ds(pl.multiple_of(source * cols, LANES), cols)],
            send_sem=send_sem.at[part, p], recv_sem=recv_sem.at[part, source],
            device_id={"rows": p}, device_id_type=MESH)

    def first_copy(p, source):
        return pltpu.make_async_remote_copy(
            src_ref=sums0, dst_ref=parts0.at[source],
            send_sem=sum0_send.at[p], recv_sem=sum0_recv.at[source],
            device_id={"rows": p}, device_id_type=MESH)

    def part_copy(g, p, source):
        e = groups[g][0]
        return pltpu.make_async_remote_copy(
            src_ref=sums.at[:, p % quarter, e], dst_ref=parts.at[source % half, :, e],
            send_sem=part_send.at[g, p % quarter], recv_sem=part_recv.at[g, source % half],
            device_id={"rows": p}, device_id_type=MESH)

    def half_copy(g):
        e = groups[g][0]
        return pltpu.make_async_remote_copy(
            src_ref=halves.at[0, :, e], dst_ref=halves.at[1, :, e],
            send_sem=half_send.at[g], recv_sem=half_recv.at[g],
            device_id={"rows": peer(half + quarter)}, device_id_type=MESH)

    def total_copy(g, p, source):
        e, at = groups[g][0], source % quarter
        return pltpu.make_async_remote_copy(
            src_ref=totals.at[:, at, e], dst_ref=totals.at[:, at, e],
            send_sem=tot_send.at[g, p % half], recv_sem=tot_recv.at[g, at],
            device_id={"rows": p}, device_id_type=MESH)

    def send_sums(g):
        each_outer(lambda p: part_copy(g, p, me).start())

    def cross_sums(g):
        @pl.when(outer)
        def _():
            e = groups[g][0]
            parts[me % half, :, e] = sums[:, place, e]
            each_beside(lambda p: part_copy(g, p, p).wait_recv())
            total = parts[0, :, e]
            for r in range(1, half):
                total = total + parts[r, :, e]
            halves[0, :, e] = total
            half_copy(g).start()

    def send_totals(g):
        @pl.when(outer)
        def _():
            e = groups[g][0]
            half_copy(g).wait_recv()
            totals[:, place, e] = (halves[0, :, e] + halves[1, :, e]) / (cols * n)
            each_beside(lambda p: total_copy(g, p, me).start())

    def take_totals(g):
        each_outer(lambda p: total_copy(g, p, p).wait_recv())

    def row_copy(p, source):
        return pltpu.make_async_remote_copy(
            src_ref=routed.at[mine, source], dst_ref=routed.at[mine, source],
            send_sem=row_send.at[p], recv_sem=row_recv.at[source],
            device_id={"rows": p}, device_id_type=MESH)

    def col_copy(q, source):
        return pltpu.make_async_remote_copy(
            src_ref=routed.at[source], dst_ref=routed.at[source],
            send_sem=col_send.at[q], recv_sem=col_recv.at[source],
            device_id={"owner": q}, device_id_type=MESH)

    def send_crossing(part, k):
        @pl.when(inner & (k >= half) & (k < end(part)) & ((k - half) // quarter == mine % 2 if part else True))
        def _():
            block_copy(part, peer(k), me).start()

    def end(part):
        return half + quarter if part == last else n

    def send_late(parts, low, high):
        for part in parts:
            @pl.loop(low, high)
            def _(k, part=part):
                block_copy(part, peer(k), me).start()

    @pl.loop(0, n)
    def _(k):
        for copy in first_loads(k):
            copy.start()

    sums[...] = jnp.zeros_like(sums)
    routed[mine, me] = (rw_ref[...] * gain_ref[...]).astype(jnp.bfloat16)

    @pl.loop(0, n)
    def _(k):
        for copy in first_loads(k):
            copy.wait()
        for j, at, size in pieces(0, first):
            span = pl.ds(pl.multiple_of((k % 2) * first + at, LANES), size)
            sums0[j, pl.ds(peer(k), 1), :] = row_sums(k // 2, span)

    pl.semaphore_wait(barrier, n - 1 + owners - 1)
    each_peer(lambda p: first_copy(p, me).start())
    parts0[me] = sums0[...]
    each_peer(lambda p: row_copy(p, me).start())
    each_peer(lambda p: first_copy(p, p).wait_recv())
    total = parts0[0]
    for r in range(1, n):
        total = total + parts0[r]
    totals0[...] = total / (cols * n)

    @pl.loop(0, n)
    def _(step):
        k = order(step)
        narrow(0, 0, first, k, k // 2, (k % 2) * first, lambda p, j: totals0[j, pl.ds(p, 1), :])
        send_crossing(0, k)

    def add_up(g, behind):
        e, low, high = groups[g]

        def body(k, step):
            p = peer(k)
            for j, at, size in pieces(low, high):
                sums[p // quarter, p % quarter, e, j:j + 1, 0:size] = row_sums(step % DEPTH, pl.ds(at - low, size))
            if behind is not None:
                pl.when(step == n // 2 - 1)(lambda: cross_sums(behind))
                pl.when(step == n - 1)(lambda: send_totals(behind))

        stream(groups[g], body)

    def narrow_all(g):
        e, low, high = groups[g]

        def body(k, step):
            narrow(e, low, high, k, step % DEPTH, 0,
                   lambda p, j: totals[p // quarter, p % quarter, e, j:j + 1, :])
            for part in parts_of(g):
                send_crossing(part, k)

        stream(groups[g], body)

    prime(groups[0])
    add_up(0, None)
    for g in range(experts):
        send_sums(g)
        if g + 1 < experts:
            prime(groups[g + 1])
            add_up(g + 1, g)
        else:
            cross_sums(g)
            send_totals(g)
        prime(groups[g])
        take_totals(g)
        narrow_all(g)

    for i in range(quarter):
        kept[i] = staged[experts - 1, rows_of(peer(half + quarter + i), cuts[2], block - cuts[2]), :]

    @pl.when(inner)
    def _():
        send_late([*range(1, last - 1)], half + quarter - turn, n - turn)
        send_late([last], half + quarter - turn, half + quarter)
        send_late([last - 1], half + quarter - turn, n - turn)

    send_late(range(last + 1), 1, half)

    each_peer(lambda p: row_copy(p, p).wait_recv())
    each_owner(lambda q: col_copy(q, mine).start())

    @pl.when(outer)
    def _():
        @pl.loop(0, 2)
        def _(i):
            begin = half + (quarter * i + turn) % half
            send_late(range(last - 2), begin, begin + quarter)

            @pl.when(begin == half)
            def _():
                send_late(range(last - 2, last + 1), half, half + quarter)

    each_owner(lambda q: col_copy(q, q).wait_recv())

    @pl.when(inner)
    def _():
        block_copy(last - 1, peer(n - turn - 2), me).wait_send()
        pl.semaphore_signal(turn_sem, inc=1, device_id={"rows": peer(quarter)}, device_id_type=MESH)

    @pl.when(outer)
    def _():
        pl.semaphore_wait(turn_sem, 1)
        send_late(range(last - 2, last + 1), half + quarter, n)

    each_owner(lambda q: col_copy(q, mine).wait_send())
    each_peer(lambda p: row_copy(p, me).wait_send())
    each_peer(lambda p: first_copy(p, me).wait_send())
    for g in range(experts):
        each_outer(lambda p, g=g: part_copy(g, p, me).wait_send())

        @pl.when(outer)
        def _(g=g):
            half_copy(g).wait_send()
            each_beside(lambda p: total_copy(g, p, me).wait_send())
    for part in range(last + 1):
        @pl.loop(1, n)
        def _(k, part=part):
            p = peer(k)

            @pl.when(outer | (k < end(part)))
            def _():
                if part == last - 1:
                    pl.when(outer | (k != n - turn - 2))(lambda: block_copy(part, p, me).wait_send())
                else:
                    block_copy(part, p, me).wait_send()
                block_copy(part, p, p).wait_recv()


def swap(n, after_ref, kept, got, send_sem, recv_sem):
    me = lax.axis_index("rows")
    half, quarter = n // 2, n // 4

    def peer(k):
        return flipped(n, me, k)

    def copy(i):
        return pltpu.make_async_remote_copy(
            src_ref=kept.at[i], dst_ref=got.at[i], send_sem=send_sem.at[i], recv_sem=recv_sem.at[i],
            device_id={"rows": peer(half + quarter + i)}, device_id_type=MESH)

    @pl.when((me // quarter) % 2 != me // half)
    def _():
        barrier = pltpu.get_barrier_semaphore()
        for i in range(quarter):
            pl.semaphore_signal(barrier, inc=1, device_id={"rows": peer(half + quarter + i)}, device_id_type=MESH)
        pl.semaphore_wait(barrier, quarter)
        for i in range(quarter):
            copy(i).start()
        for i in range(quarter):
            copy(i).wait()


def place(n, low, out_in, got, out_ref, sem):
    me = lax.axis_index("rows")
    quarter = n // 4
    experts, block, _ = out_ref.shape
    cols = got.shape[2]

    @pl.when((me // quarter) % 2 != me // (n // 2))
    def _():
        copies = []
        for i in range(quarter):
            source = flipped(n, me, n - quarter + i)
            copies.append(pltpu.make_async_copy(
                got.at[i], out_ref.at[experts - 1, pl.ds(low, block - low), pl.ds(pl.multiple_of(source * cols, LANES), cols)],
                sem.at[i]))
        for copy in copies:
            copy.start()
        for copy in copies:
            copy.wait()


def finish(first, held, totals, totals0, routed, out_ref, scale_ref, router_ref, done, scale, wide, router, out_sem, sem):
    me = lax.axis_index("rows")
    experts, block, _ = held.shape
    owners, n, few, cols = routed.shape
    quarter = totals.shape[1]
    outs = [pltpu.make_async_copy(held.at[e], out_ref.at[e], out_sem.at[e]) for e in range(experts)]
    for copy in outs:
        copy.start()
    for e in range(experts):
        for j, at, size in pieces(0, block):
            if e == 0 and at < first:
                row = totals0[j, pl.ds(me, 1), :]
            else:
                row = totals[me // quarter, me % quarter, e, j:j + 1, 0:size]
            scale[e:e + 1, at:at + size] = row
    for q in range(owners):
        for r in range(n):
            wide[q * few:(q + 1) * few, r * cols:(r + 1) * cols] = routed[q, r].astype(jnp.float32)
    router[...] = wide[...].astype(jnp.bfloat16)
    small = [pltpu.make_async_copy(scale, scale_ref, sem.at[0]), pltpu.make_async_copy(router, router_ref, sem.at[1])]
    for copy in small:
        copy.start()
    for copy in small + outs:
        copy.wait()
    done[...] = jnp.zeros_like(done)


def with_kernel(n, owners, w_down, avg_down, router_weight, router_gain):
    experts, rows, cols = w_down.shape
    few = router_weight.shape[1]
    block = rows // n
    half, quarter = n // 2, n // 4
    piece = -(-block // LANES)
    first = LANES * min(2, (block - 1) // LANES)
    middle = block // 2 // LANES * LANES
    cuts = (middle - LANES, middle, middle + LANES)
    tail = pltpu.VMEM((quarter, block - cuts[2], cols), jnp.bfloat16)
    dma = pltpu.SemaphoreType.DMA
    anywhere, vmem = pl.BlockSpec(memory_space=pl.ANY), pl.BlockSpec(memory_space=pltpu.VMEM)
    sums = pltpu.VMEM((4, quarter, experts, piece, LANES), jnp.float32)
    sums0 = pltpu.VMEM((first // LANES, n, LANES), jnp.float32)
    *held, kept = pl.pallas_call(
        functools.partial(kernel, n, owners, first, cuts),
        out_shape=(
            pltpu.VMEM((experts, block, cols * n), jnp.bfloat16),
            sums,
            sums0,
            pltpu.VMEM((owners, n, few, cols), jnp.bfloat16),
            tail,
        ),
        in_specs=[anywhere] * 2 + [vmem] * 2,
        out_specs=(vmem,) * 5,
        scratch_shapes=[
            pltpu.VMEM((DEPTH, block, cols), jnp.float32),
            pltpu.VMEM((DEPTH, block, cols), jnp.bfloat16),
            pltpu.VMEM((experts, rows, cols), jnp.bfloat16),
            sums,
            pltpu.VMEM((half, 4, experts, piece, LANES), jnp.float32),
            pltpu.VMEM((2, 4, experts, piece, LANES), jnp.float32),
            sums0,
            pltpu.VMEM((n, first // LANES, n, LANES), jnp.float32),
            dma((2, DEPTH)), dma((2, n)),
            dma((experts + 4, n)), dma((experts + 4, n)),
            dma((n,)), dma((n,)),
            dma((experts, quarter)), dma((experts, half)), dma((experts,)), dma((experts,)),
            dma((experts, half)), dma((experts, quarter)),
            dma((n,)), dma((n,)), dma((owners,)), dma((owners,)),
            pltpu.SemaphoreType.REGULAR,
        ],
        compiler_params=pltpu.CompilerParams(
            collective_id=0, has_side_effects=True, vmem_limit_bytes=VMEM_LIMIT
        ),
        name="serve",
    )(w_down, avg_down, router_weight.T, router_gain[None, :])
    out, scales, router, done = pl.pallas_call(
        functools.partial(finish, first),
        out_shape=(
            jax.ShapeDtypeStruct((experts, block, cols * n), jnp.bfloat16),
            jax.ShapeDtypeStruct((experts, block), jnp.float32),
            jax.ShapeDtypeStruct((owners * few, cols * n), jnp.bfloat16),
            pltpu.VMEM((8, LANES), jnp.float32),
        ),
        in_specs=[vmem] * 4,
        out_specs=(anywhere,) * 3 + (vmem,),
        scratch_shapes=[
            pltpu.VMEM((experts, block), jnp.float32),
            pltpu.VMEM((owners * few, cols * n), jnp.float32),
            pltpu.VMEM((owners * few, cols * n), jnp.bfloat16),
            dma((experts,)), dma((2,)),
        ],
        compiler_params=pltpu.CompilerParams(vmem_limit_bytes=4 * 1024 * 1024),
        name="finish",
    )(*held)
    got = pl.pallas_call(
        functools.partial(swap, n),
        out_shape=tail,
        in_specs=[vmem, vmem],
        out_specs=vmem,
        scratch_shapes=[dma((quarter,)), dma((quarter,))],
        compiler_params=pltpu.CompilerParams(
            collective_id=1, has_side_effects=True, vmem_limit_bytes=1024 * 1024
        ),
        name="swap",
    )(done, kept)
    out = pl.pallas_call(
        functools.partial(place, n, cuts[2]),
        out_shape=jax.ShapeDtypeStruct(out.shape, out.dtype),
        in_specs=[anywhere, vmem],
        out_specs=anywhere,
        scratch_shapes=[dma((quarter,))],
        input_output_aliases={0: 0},
        compiler_params=pltpu.CompilerParams(vmem_limit_bytes=1024 * 1024),
        name="place",
    )(out, got)
    return out, scales, router.T


def with_collectives(n, owners, w_down, avg_down, router_weight, router_gain):
    fresh = w_down + avg_down.astype(jnp.float32)
    scales = lax.psum(jnp.sum(jnp.abs(fresh), axis=2), "rows") / (w_down.shape[2] * n)
    narrow = (fresh / jnp.expand_dims(scales, 2)).astype(jnp.bfloat16)
    out = lax.all_to_all(narrow, "rows", split_axis=1, concat_axis=2, tiled=True)
    scales = lax.dynamic_slice_in_dim(scales, lax.axis_index("rows") * out.shape[1], out.shape[1], axis=1)
    part = (router_weight * router_gain[:, None]).astype(jnp.bfloat16)
    router = lax.all_gather(lax.all_gather(part, "rows", axis=0, tiled=True), "owner", axis=1, tiled=True)
    return out, scales, router


def solution(mesh):
    n, owners = mesh.shape["rows"], mesh.shape["owner"]

    def per_device(w_down, avg_down, router_weight, router_gain):
        experts, rows, cols = w_down.shape
        fits = n >= 8 and (n & (n - 1)) == 0 and rows // n >= 4 * LANES and rows % LANES == 0 and rows % (16 * n) == 0 and cols % LANES == 0
        path = with_kernel if fits else with_collectives
        return path(n, owners, w_down, avg_down, router_weight, router_gain)

    return jax.shard_map(
        per_device,
        mesh=mesh,
        in_specs=(
            P("owner", None, "rows"),
            P("owner", None, "rows"),
            P("rows", "owner"),
            P("rows"),
        ),
        out_specs=(P("owner", "rows", None), P("owner", "rows"), P()),
        check_vma=False,
    )
```

```python
import functools

import jax
import jax.numpy as jnp
from jax import lax
from jax.experimental import pallas as pl
from jax.experimental.pallas import tpu as pltpu
from jax.sharding import PartitionSpec as P

LANES = 128
DEPTH = 4
VMEM_LIMIT = 36 * 1024 * 1024
MESH = pl.DeviceIdType.MESH


def pieces(low, high):
    return [(at // LANES, at, min(LANES, high - at)) for at in range(low, high, LANES)]


def flipped(n, me, k):
    out, bit = 0, 1
    while bit < n:
        out = out + bit * (((me // bit) % 2 + (k // bit) % 2) % 2)
        bit *= 2
    return out


def kernel(n, owners, first, cuts, w_ref, a_ref, rw_ref, gain_ref, out_ref, totals, totals0, routed, kept,
           w_buf, a_buf, staged, sums, parts, halves, sums0, parts0,
           load_sem, load0_sem, send_sem, recv_sem, sum0_send, sum0_recv,
           part_send, part_recv, half_send, half_recv, tot_send, tot_recv,
           row_send, row_recv, col_send, col_recv, turn_sem, both_sem):
    me, mine = lax.axis_index("rows"), lax.axis_index("owner")
    experts, rows, cols = w_ref.shape
    block = rows // n
    half, quarter = n // 2, n // 4
    side, place = me // half, me % quarter
    outer = (me // quarter) % 2 == side
    inner = (me // quarter) % 2 != side
    turn = (mine % 2) * quarter
    groups = [(0, first, block)] + [(e, 0, block) for e in range(1, experts)]
    e = experts - 1
    last = experts + 3
    spans = [(0, 0, first)] + groups[:-1] + [(e, low, high) for low, high in zip((groups[-1][1],) + cuts, cuts + (block,))]
    parts_of = lambda g: range(experts, last + 1) if g == experts - 1 else [g + 1]

    def peer(k):
        return flipped(n, me, k)

    def each_peer(fn):
        @pl.loop(1, n)
        def _(k):
            fn(peer(k))

    def each_owner(fn):
        @pl.loop(1, owners)
        def _(k):
            fn((mine + k) % owners)

    def each_outer(fn):
        @pl.loop(0, quarter)
        def _(i):
            p = side * (half + quarter) + i
            pl.when(p != me)(lambda: fn(p))

    def each_beside(fn):
        @pl.loop(1, half)
        def _(k):
            fn(peer(k))

    barrier = pltpu.get_barrier_semaphore()
    each_peer(lambda p: pl.semaphore_signal(barrier, inc=1, device_id={"rows": p}, device_id_type=MESH))
    each_owner(lambda q: pl.semaphore_signal(barrier, inc=1, device_id={"owner": q}, device_id_type=MESH))

    def rows_of(p, low, count):
        return pl.ds(pl.multiple_of(p * block + low, 16), count)

    def first_loads(k):
        span = rows_of(peer(k), 0, first)
        to = pl.ds(pl.multiple_of((k % 2) * first, LANES), first)
        return (pltpu.make_async_copy(w_ref.at[0, span], w_buf.at[k // 2, to], load0_sem.at[0, k]),
                pltpu.make_async_copy(a_ref.at[0, span], a_buf.at[k // 2, to], load0_sem.at[1, k]))

    def loads(e, low, high, step):
        slot, span, to = step % DEPTH, rows_of(peer(order(step)), low, high - low), pl.ds(0, high - low)
        return (pltpu.make_async_copy(w_ref.at[e, span], w_buf.at[slot, to], load_sem.at[0, slot]),
                pltpu.make_async_copy(a_ref.at[e, span], a_buf.at[slot, to], load_sem.at[1, slot]))

    def order(step):
        return jnp.where(step < half, half + (step + turn) % half, step - half)

    def prime(group):
        for step in range(min(DEPTH - 1, n)):
            for copy in loads(*group, step):
                copy.start()

    def stream(group, body):
        @pl.loop(0, n)
        def _(step):
            for copy in loads(*group, step):
                copy.wait()

            @pl.when(step + (DEPTH - 1) < n)
            def _():
                for copy in loads(*group, step + (DEPTH - 1)):
                    copy.start()

            body(order(step), step)

    def fresh(slot, span, c):
        return w_buf[slot, span, c:c + LANES] + a_buf[slot, span, c:c + LANES].astype(jnp.float32)

    def row_sums(slot, span):
        acc = None
        for c in range(0, cols, LANES):
            f = jnp.abs(fresh(slot, span, c))
            acc = f if acc is None else acc + f
        return jnp.sum(acc.T, axis=0, keepdims=True)

    def narrow(e, low, high, k, slot, start, total):
        p = peer(k)

        def write(put):
            for j, at, size in pieces(low, high):
                factor = jnp.broadcast_to(1.0 / total(p, j), (LANES, LANES)).T[:size]
                span = pl.ds(pl.multiple_of(start + (at - low), LANES), size)
                for c in range(0, cols, LANES):
                    put(at, size, c, (fresh(slot, span, c) * factor).astype(jnp.bfloat16))

        def keep(at, size, c, value):
            out_ref[e, at:at + size, pl.ds(pl.multiple_of(me * cols + c, LANES), LANES)] = value

        def stage(at, size, c, value):
            staged[e, rows_of(p, at, size), c:c + LANES] = value

        pl.when(k == 0)(lambda: write(keep))
        pl.when(k != 0)(lambda: write(stage))

    def block_copy(part, p, source):
        e, low, high = spans[part]
        return pltpu.make_async_remote_copy(
            src_ref=staged.at[e, rows_of(p, low, high - low)],
            dst_ref=out_ref.at[e, pl.ds(low, high - low), pl.ds(pl.multiple_of(source * cols, LANES), cols)],
            send_sem=send_sem.at[part, p], recv_sem=recv_sem.at[part, source],
            device_id={"rows": p}, device_id_type=MESH)

    def first_copy(p, source):
        return pltpu.make_async_remote_copy(
            src_ref=sums0, dst_ref=parts0.at[source],
            send_sem=sum0_send.at[p], recv_sem=sum0_recv.at[source],
            device_id={"rows": p}, device_id_type=MESH)

    def part_copy(g, p, source):
        e = groups[g][0]
        return pltpu.make_async_remote_copy(
            src_ref=sums.at[:, p % quarter, e], dst_ref=parts.at[source % half, :, e],
            send_sem=part_send.at[g, p % quarter], recv_sem=part_recv.at[g, source % half],
            device_id={"rows": p}, device_id_type=MESH)

    def half_copy(g):
        e = groups[g][0]
        return pltpu.make_async_remote_copy(
            src_ref=halves.at[0, :, e], dst_ref=halves.at[1, :, e],
            send_sem=half_send.at[g], recv_sem=half_recv.at[g],
            device_id={"rows": peer(half + quarter)}, device_id_type=MESH)

    def total_copy(g, p, source):
        e, at = groups[g][0], source % quarter
        return pltpu.make_async_remote_copy(
            src_ref=totals.at[:, at, e], dst_ref=totals.at[:, at, e],
            send_sem=tot_send.at[g, p % half], recv_sem=tot_recv.at[g, at],
            device_id={"rows": p}, device_id_type=MESH)

    def send_sums(g):
        each_outer(lambda p: part_copy(g, p, me).start())

    def cross_sums(g):
        @pl.when(outer)
        def _():
            e = groups[g][0]
            parts[me % half, :, e] = sums[:, place, e]
            each_beside(lambda p: part_copy(g, p, p).wait_recv())
            total = parts[0, :, e]
            for r in range(1, half):
                total = total + parts[r, :, e]
            halves[0, :, e] = total
            half_copy(g).start()

    def send_totals(g):
        @pl.when(outer)
        def _():
            e = groups[g][0]
            half_copy(g).wait_recv()
            totals[:, place, e] = (halves[0, :, e] + halves[1, :, e]) / (cols * n)
            each_beside(lambda p: total_copy(g, p, me).start())

    def take_totals(g):
        each_outer(lambda p: total_copy(g, p, p).wait_recv())

    def row_copy(p, source):
        return pltpu.make_async_remote_copy(
            src_ref=routed.at[mine, source], dst_ref=routed.at[mine, source],
            send_sem=row_send.at[p], recv_sem=row_recv.at[source],
            device_id={"rows": p}, device_id_type=MESH)

    def col_copy(q, source):
        return pltpu.make_async_remote_copy(
            src_ref=routed.at[source], dst_ref=routed.at[source],
            send_sem=col_send.at[q], recv_sem=col_recv.at[source],
            device_id={"owner": q}, device_id_type=MESH)

    def send_crossing(part, k):
        @pl.when(inner & (k >= half) & (k < end(part)) & ((k - half) // quarter == mine % 2 if part else True))
        def _():
            block_copy(part, peer(k), me).start()

    def end(part):
        return half + quarter if part == last else n

    def send_late(parts, low, high):
        for part in parts:
            @pl.loop(low, high)
            def _(k, part=part):
                block_copy(part, peer(k), me).start()

    @pl.loop(0, n)
    def _(k):
        for copy in first_loads(k):
            copy.start()

    sums[...] = jnp.zeros_like(sums)
    routed[mine, me] = (rw_ref[...] * gain_ref[...]).astype(jnp.bfloat16)

    @pl.loop(0, n)
    def _(k):
        for copy in first_loads(k):
            copy.wait()
        for j, at, size in pieces(0, first):
            span = pl.ds(pl.multiple_of((k % 2) * first + at, LANES), size)
            sums0[j, pl.ds(peer(k), 1), :] = row_sums(k // 2, span)

    pl.semaphore_wait(barrier, n - 1 + owners - 1)
    each_peer(lambda p: first_copy(p, me).start())
    parts0[me] = sums0[...]
    each_peer(lambda p: row_copy(p, me).start())
    each_peer(lambda p: first_copy(p, p).wait_recv())
    total = parts0[0]
    for r in range(1, n):
        total = total + parts0[r]
    totals0[...] = total / (cols * n)

    @pl.loop(0, n)
    def _(step):
        k = order(step)
        narrow(0, 0, first, k, k // 2, (k % 2) * first, lambda p, j: totals0[j, pl.ds(p, 1), :])
        send_crossing(0, k)

    def add_up(g, behind):
        e, low, high = groups[g]

        def body(k, step):
            p = peer(k)
            for j, at, size in pieces(low, high):
                sums[p // quarter, p % quarter, e, j:j + 1, 0:size] = row_sums(step % DEPTH, pl.ds(at - low, size))
            if behind is not None:
                pl.when(step == n // 2 - 1)(lambda: cross_sums(behind))
                pl.when(step == n - 1)(lambda: send_totals(behind))

        stream(groups[g], body)

    def narrow_all(g):
        e, low, high = groups[g]

        def body(k, step):
            narrow(e, low, high, k, step % DEPTH, 0,
                   lambda p, j: totals[p // quarter, p % quarter, e, j:j + 1, :])
            for part in parts_of(g):
                send_crossing(part, k)

        stream(groups[g], body)

    prime(groups[0])
    add_up(0, None)
    for g in range(experts):
        send_sums(g)
        if g + 1 < experts:
            prime(groups[g + 1])
            add_up(g + 1, g)
        else:
            cross_sums(g)
            send_totals(g)
        prime(groups[g])
        take_totals(g)
        narrow_all(g)

    for i in range(quarter):
        kept[i] = staged[experts - 1, rows_of(peer(half + quarter + i), cuts[2], block - cuts[2]), :]

    @pl.when(inner)
    def _():
        send_late([*range(1, last - 1)], half + quarter - turn, n - turn)
        send_late([last], half + quarter - turn, half + quarter)
        send_late([last - 1], half + quarter - turn, n - turn)

    send_late(range(last + 1), 1, half)

    each_peer(lambda p: row_copy(p, p).wait_recv())
    each_owner(lambda q: col_copy(q, mine).start())

    @pl.when(outer)
    def _():
        @pl.loop(0, 2)
        def _(i):
            begin = half + (quarter * i + turn) % half
            send_late(range(last - 2), begin, begin + quarter)

            @pl.when(begin == half)
            def _():
                send_late(range(last - 2, last + 1), half, half + quarter)

    each_owner(lambda q: col_copy(q, q).wait_recv())

    @pl.when(inner)
    def _():
        block_copy(last - 1, peer(n - turn - 2), me).wait_send()
        pl.semaphore_signal(both_sem, inc=1, device_id={"owner": mine + 1 - 2 * (mine % 2)}, device_id_type=MESH)
        pl.semaphore_wait(both_sem, 1)
        pl.semaphore_signal(turn_sem, inc=1, device_id={"rows": peer(quarter)}, device_id_type=MESH)

    @pl.when(outer)
    def _():
        pl.semaphore_wait(turn_sem, 1)
        send_late(range(last - 2, last + 1), half + quarter, n)

    each_owner(lambda q: col_copy(q, mine).wait_send())
    each_peer(lambda p: row_copy(p, me).wait_send())
    each_peer(lambda p: first_copy(p, me).wait_send())
    for g in range(experts):
        each_outer(lambda p, g=g: part_copy(g, p, me).wait_send())

        @pl.when(outer)
        def _(g=g):
            half_copy(g).wait_send()
            each_beside(lambda p: total_copy(g, p, me).wait_send())
    for part in range(last + 1):
        @pl.loop(1, n)
        def _(k, part=part):
            p = peer(k)

            @pl.when(outer | (k < end(part)))
            def _():
                if part == last - 1:
                    pl.when(outer | (k != n - turn - 2))(lambda: block_copy(part, p, me).wait_send())
                else:
                    block_copy(part, p, me).wait_send()
                block_copy(part, p, p).wait_recv()


def swap(n, after_ref, kept, got, send_sem, recv_sem):
    me = lax.axis_index("rows")
    half, quarter = n // 2, n // 4

    def peer(k):
        return flipped(n, me, k)

    def copy(i):
        return pltpu.make_async_remote_copy(
            src_ref=kept.at[i], dst_ref=got.at[i], send_sem=send_sem.at[i], recv_sem=recv_sem.at[i],
            device_id={"rows": peer(half + quarter + i)}, device_id_type=MESH)

    @pl.when((me // quarter) % 2 != me // half)
    def _():
        barrier = pltpu.get_barrier_semaphore()
        for i in range(quarter):
            pl.semaphore_signal(barrier, inc=1, device_id={"rows": peer(half + quarter + i)}, device_id_type=MESH)
        pl.semaphore_wait(barrier, quarter)
        for i in range(quarter):
            copy(i).start()
        for i in range(quarter):
            copy(i).wait()


def place(n, low, out_in, got, out_ref, sem):
    me = lax.axis_index("rows")
    quarter = n // 4
    experts, block, _ = out_ref.shape
    cols = got.shape[2]

    @pl.when((me // quarter) % 2 != me // (n // 2))
    def _():
        copies = []
        for i in range(quarter):
            source = flipped(n, me, n - quarter + i)
            copies.append(pltpu.make_async_copy(
                got.at[i], out_ref.at[experts - 1, pl.ds(low, block - low), pl.ds(pl.multiple_of(source * cols, LANES), cols)],
                sem.at[i]))
        for copy in copies:
            copy.start()
        for copy in copies:
            copy.wait()


def finish(first, held, totals, totals0, routed, out_ref, scale_ref, router_ref, done, scale, wide, router, out_sem, sem):
    me = lax.axis_index("rows")
    experts, block, _ = held.shape
    owners, n, few, cols = routed.shape
    quarter = totals.shape[1]
    outs = [pltpu.make_async_copy(held.at[e], out_ref.at[e], out_sem.at[e]) for e in range(experts)]
    for copy in outs:
        copy.start()
    for e in range(experts):
        for j, at, size in pieces(0, block):
            if e == 0 and at < first:
                row = totals0[j, pl.ds(me, 1), :]
            else:
                row = totals[me // quarter, me % quarter, e, j:j + 1, 0:size]
            scale[e:e + 1, at:at + size] = row
    for q in range(owners):
        for r in range(n):
            wide[q * few:(q + 1) * few, r * cols:(r + 1) * cols] = routed[q, r].astype(jnp.float32)
    router[...] = wide[...].astype(jnp.bfloat16)
    small = [pltpu.make_async_copy(scale, scale_ref, sem.at[0]), pltpu.make_async_copy(router, router_ref, sem.at[1])]
    for copy in small:
        copy.start()
    for copy in small + outs:
        copy.wait()
    done[...] = jnp.zeros_like(done)


def with_kernel(n, owners, w_down, avg_down, router_weight, router_gain):
    experts, rows, cols = w_down.shape
    few = router_weight.shape[1]
    block = rows // n
    half, quarter = n // 2, n // 4
    piece = -(-block // LANES)
    first = LANES * min(2, (block - 1) // LANES)
    middle = block // 2 // LANES * LANES
    cuts = (middle - LANES, middle + LANES - 64, middle + LANES)
    tail = pltpu.VMEM((quarter, block - cuts[2], cols), jnp.bfloat16)
    dma = pltpu.SemaphoreType.DMA
    anywhere, vmem = pl.BlockSpec(memory_space=pl.ANY), pl.BlockSpec(memory_space=pltpu.VMEM)
    sums = pltpu.VMEM((4, quarter, experts, piece, LANES), jnp.float32)
    sums0 = pltpu.VMEM((first // LANES, n, LANES), jnp.float32)
    *held, kept = pl.pallas_call(
        functools.partial(kernel, n, owners, first, cuts),
        out_shape=(
            pltpu.VMEM((experts, block, cols * n), jnp.bfloat16),
            sums,
            sums0,
            pltpu.VMEM((owners, n, few, cols), jnp.bfloat16),
            tail,
        ),
        in_specs=[anywhere] * 2 + [vmem] * 2,
        out_specs=(vmem,) * 5,
        scratch_shapes=[
            pltpu.VMEM((DEPTH, block, cols), jnp.float32),
            pltpu.VMEM((DEPTH, block, cols), jnp.bfloat16),
            pltpu.VMEM((experts, rows, cols), jnp.bfloat16),
            sums,
            pltpu.VMEM((half, 4, experts, piece, LANES), jnp.float32),
            pltpu.VMEM((2, 4, experts, piece, LANES), jnp.float32),
            sums0,
            pltpu.VMEM((n, first // LANES, n, LANES), jnp.float32),
            dma((2, DEPTH)), dma((2, n)),
            dma((experts + 4, n)), dma((experts + 4, n)),
            dma((n,)), dma((n,)),
            dma((experts, quarter)), dma((experts, half)), dma((experts,)), dma((experts,)),
            dma((experts, half)), dma((experts, quarter)),
            dma((n,)), dma((n,)), dma((owners,)), dma((owners,)),
            pltpu.SemaphoreType.REGULAR, pltpu.SemaphoreType.REGULAR,
        ],
        compiler_params=pltpu.CompilerParams(
            collective_id=0, has_side_effects=True, vmem_limit_bytes=VMEM_LIMIT
        ),
        name="serve",
    )(w_down, avg_down, router_weight.T, router_gain[None, :])
    out, scales, router, done = pl.pallas_call(
        functools.partial(finish, first),
        out_shape=(
            jax.ShapeDtypeStruct((experts, block, cols * n), jnp.bfloat16),
            jax.ShapeDtypeStruct((experts, block), jnp.float32),
            jax.ShapeDtypeStruct((owners * few, cols * n), jnp.bfloat16),
            pltpu.VMEM((8, LANES), jnp.float32),
        ),
        in_specs=[vmem] * 4,
        out_specs=(anywhere,) * 3 + (vmem,),
        scratch_shapes=[
            pltpu.VMEM((experts, block), jnp.float32),
            pltpu.VMEM((owners * few, cols * n), jnp.float32),
            pltpu.VMEM((owners * few, cols * n), jnp.bfloat16),
            dma((experts,)), dma((2,)),
        ],
        compiler_params=pltpu.CompilerParams(vmem_limit_bytes=4 * 1024 * 1024),
        name="finish",
    )(*held)
    got = pl.pallas_call(
        functools.partial(swap, n),
        out_shape=tail,
        in_specs=[vmem, vmem],
        out_specs=vmem,
        scratch_shapes=[dma((quarter,)), dma((quarter,))],
        compiler_params=pltpu.CompilerParams(
            collective_id=1, has_side_effects=True, vmem_limit_bytes=1024 * 1024
        ),
        name="swap",
    )(done, kept)
    out = pl.pallas_call(
        functools.partial(place, n, cuts[2]),
        out_shape=jax.ShapeDtypeStruct(out.shape, out.dtype),
        in_specs=[anywhere, vmem],
        out_specs=anywhere,
        scratch_shapes=[dma((quarter,))],
        input_output_aliases={0: 0},
        compiler_params=pltpu.CompilerParams(vmem_limit_bytes=1024 * 1024),
        name="place",
    )(out, got)
    return out, scales, router.T


def with_collectives(n, owners, w_down, avg_down, router_weight, router_gain):
    fresh = w_down + avg_down.astype(jnp.float32)
    scales = lax.psum(jnp.sum(jnp.abs(fresh), axis=2), "rows") / (w_down.shape[2] * n)
    narrow = (fresh / jnp.expand_dims(scales, 2)).astype(jnp.bfloat16)
    out = lax.all_to_all(narrow, "rows", split_axis=1, concat_axis=2, tiled=True)
    scales = lax.dynamic_slice_in_dim(scales, lax.axis_index("rows") * out.shape[1], out.shape[1], axis=1)
    part = (router_weight * router_gain[:, None]).astype(jnp.bfloat16)
    router = lax.all_gather(lax.all_gather(part, "rows", axis=0, tiled=True), "owner", axis=1, tiled=True)
    return out, scales, router


def solution(mesh):
    n, owners = mesh.shape["rows"], mesh.shape["owner"]

    def per_device(w_down, avg_down, router_weight, router_gain):
        experts, rows, cols = w_down.shape
        fits = n >= 8 and owners % 2 == 0 and (n & (n - 1)) == 0 and rows // n >= 4 * LANES and rows % LANES == 0 and rows % (16 * n) == 0 and cols % LANES == 0
        path = with_kernel if fits else with_collectives
        return path(n, owners, w_down, avg_down, router_weight, router_gain)

    return jax.shard_map(
        per_device,
        mesh=mesh,
        in_specs=(
            P("owner", None, "rows"),
            P("owner", None, "rows"),
            P("rows", "owner"),
            P("rows"),
        ),
        out_specs=(P("owner", "rows", None), P("owner", "rows"), P()),
        check_vma=False,
    )
```
